8 devices in a mesh: dp: 2 (over z, y), tp: 4 (over x, core).
Axes of the slice: x: 2, y: 2, z: 1, core: 2. Of those that a mesh axis runs over, the one named last changes fastest.
Arguments:
- y1: float32 [4, 8, 64, 1536], P('dp'), parts along dimension 0
- y2: float32 [4, 8, 64, 1536], P('dp'), parts along dimension 0
- dy1: float32 [4, 8, 64, 1536], P('dp'), parts along dimension 0
- dy2: float32 [4, 8, 64, 1536], P('dp'), parts along dimension 0
- w_qkv: bfloat16 [4, 1536, 3, 16, 96], P(None, None, None, 'tp')
- w_out: bfloat16 [4, 16, 96, 1536], P(None, 'tp')
- w_up: bfloat16 [4, 1536, 6144], P(None, None, 'tp')
- w_down: bfloat16 [4, 6144, 1536], P(None, 'tp')
Outputs:
- output 1: float32 [4, 8, 64, 1536], P('dp'), parts along dimension 0
- output 2: float32 [4, 8, 64, 1536], P('dp'), parts along dimension 0
- output 3: float32 [4, 8, 64, 1536], P('dp'), parts along dimension 0
- output 4: float32 [4, 8, 64, 1536], P('dp'), parts along dimension 0
- output 5: float32 [8, 1536, 3, 16, 96], P('dp', None, None, 'tp'), parts along dimension 0
- output 6: float32 [8, 16, 96, 1536], P('dp', 'tp'), parts along dimension 0
- output 7: float32 [8, 1536, 6144], P('dp', None, 'tp'), parts along dimension 0
- output 8: float32 [8, 6144, 1536], P('dp', 'tp'), parts along dimension 0
There are 2 independent parts. The reference program is written for one: setup_inputs(seed, part) draws one part's arguments, and reference() takes and returns one part's arrays. A program takes and returns all parts, laid end to end along the dimension named above; an argument that names none is the same for every part.
All inputs are finite; a program needn't handle non-finite values.
Results may differ from the reference program's by a relative error of at most 0.0111179.
Values are sent between devices in bfloat16 or wider.
A program may use at most 1 GiB of HBM per device.

```python
import jax
import jax.numpy as jnp
from jax import lax

H = 1536
HEADS = 16
FF = 6144
BATCH = 8
SEQ = 64
LAYERS = 4
HEAD_DIM = H // HEADS
EPS = 1e-6


def setup_inputs(seed: int = 0, part: int = 0) -> dict:
    part_key = jax.random.fold_in(jax.random.key(seed), part)
    key_tok, key_seq, key_grad = jax.random.split(part_key, 3)
    act_shape = (2, 2, BATCH, SEQ, H)
    tok_noise = jax.random.normal(key_tok, act_shape, jnp.float32)
    seq_shared = jax.random.normal(key_seq, (2, 2, BATCH, 1, H), jnp.float32)
    y_pair = 0.8 * tok_noise + 0.6 * seq_shared
    dy_pair = jax.random.normal(key_grad, act_shape, jnp.float32)
    key_qkv, key_out, key_up, key_down = jax.random.split(jax.random.key(seed + 1), 4)
    branch_gain = (LAYERS + 2) ** -0.5
    w_qkv = jax.random.normal(key_qkv, (LAYERS, H, 3, HEADS, HEAD_DIM), jnp.float32) * H ** -0.5
    w_out = jax.random.normal(key_out, (LAYERS, HEADS, HEAD_DIM, H), jnp.float32) * (branch_gain * H ** -0.5)
    w_up = jax.random.normal(key_up, (LAYERS, H, FF), jnp.float32) * H ** -0.5
    w_down = jax.random.normal(key_down, (LAYERS, FF, H), jnp.float32) * (branch_gain * FF ** -0.5)
    return {'y1': y_pair[0], 'y2': y_pair[1], 'dy1': dy_pair[0], 'dy2': dy_pair[1],
            'w_qkv': w_qkv.astype(jnp.bfloat16), 'w_out': w_out.astype(jnp.bfloat16),
            'w_up': w_up.astype(jnp.bfloat16), 'w_down': w_down.astype(jnp.bfloat16)}


def to_bf16(value):
    return value.astype(jnp.bfloat16).astype(jnp.float32)


def rms_norm(x_in):
    return x_in * lax.rsqrt(jnp.mean(x_in * x_in, axis=-1, keepdims=True) + EPS)


def attend_one(qkv_seq):
    scores = jnp.einsum('qnd,knd->nqk', qkv_seq[0], qkv_seq[1]) * HEAD_DIM ** -0.5
    prob_half = to_bf16(jax.nn.softmax(scores, axis=-1))
    return to_bf16(jnp.einsum('nqk,knd->qnd', prob_half, qkv_seq[2]))


def branch_f(x_in, w_qkv, w_out):
    normed = to_bf16(rms_norm(x_in))
    qkv_all = to_bf16(jnp.einsum('rsh,hcnd->rcsnd', normed, w_qkv))
    attn_out = lax.map(jax.checkpoint(attend_one), qkv_all)
    return jnp.einsum('rsnd,ndh->rsh', attn_out, w_out)


def branch_g(x_in, w_up, w_down):
    normed = to_bf16(rms_norm(x_in))
    act_half = to_bf16(jax.nn.gelu(jnp.einsum('rsh,hf->rsf', normed, w_up)))
    return jnp.einsum('rsf,fh->rsh', act_half, w_down)


def reference(y1, y2, dy1, dy2, w_qkv, w_out, w_up, w_down):
    row_shape = (2 * BATCH, SEQ, H)

    def block_step(carry, weights):
        upper_one, upper_two, grad_one, grad_two = carry
        layer_qkv, layer_out, layer_up, layer_down = [weight.astype(jnp.float32) for weight in weights]
        g_val, g_pull = jax.vjp(branch_g, upper_one, layer_up, layer_down)
        lower_two = upper_two - g_val
        g_in, g_up, g_down = g_pull(grad_two)
        grad_one = grad_one + g_in
        f_val, f_pull = jax.vjp(branch_f, lower_two, layer_qkv, layer_out)
        lower_one = upper_one - f_val
        f_in, f_qkv, f_out = f_pull(grad_one)
        return (lower_one, lower_two, grad_one, grad_two + f_in), (f_qkv, f_out, g_up, g_down)

    start_carry = (y1.reshape(row_shape), y2.reshape(row_shape), dy1.reshape(row_shape), dy2.reshape(row_shape))
    layer_weights = (w_qkv[::-1], w_out[::-1], w_up[::-1], w_down[::-1])
    final_carry, grad_stack = lax.scan(block_step, start_carry, layer_weights)
    out_shape = (2, BATCH, SEQ, H)
    return (final_carry[0].reshape(out_shape), final_carry[1].reshape(out_shape),
            final_carry[2].reshape(out_shape), final_carry[3].reshape(out_shape),
            grad_stack[0][::-1], grad_stack[1][::-1], grad_stack[2][::-1], grad_stack[3][::-1])
```

```python
import jax
import jax.numpy as jnp
from jax import lax
from jax.sharding import PartitionSpec as P

EPS = 1e-6
STREAMS = 2
BF16 = jnp.bfloat16
F32 = jnp.float32


def rms_norm(x_in):
    return x_in * lax.rsqrt(jnp.mean(x_in * x_in, axis=-1, keepdims=True) + EPS)


def norm_back(x_in, grad_norm):
    return jax.vjp(rms_norm, x_in)[1](grad_norm)[0]


def mlp_forward(normed, w_up, w_down):
    up_pre = jnp.einsum('rsh,hf->rsf', normed, w_up, preferred_element_type=F32)
    act_full, gelu_pull = jax.vjp(jax.nn.gelu, up_pre)
    act_half = act_full.astype(BF16)
    part_out = jnp.einsum('rsf,fh->rsh', act_half, w_down, preferred_element_type=F32)
    return part_out, (act_half, gelu_pull)


def mlp_backward(grad_half, saved_mlp, w_up, w_down):
    act_half, gelu_pull = saved_mlp
    d_act = jnp.einsum('rsh,fh->rsf', grad_half, w_down, preferred_element_type=F32)
    d_pre = gelu_pull(d_act)[0].astype(BF16)
    norm_part = jnp.einsum('rsf,hf->rsh', d_pre, w_up, preferred_element_type=F32)
    return norm_part.astype(BF16), d_pre


def attn_forward(normed, w_qkv, w_out):
    qkv_all = jnp.einsum('rsh,hcnd->crsnd', normed, w_qkv, preferred_element_type=F32).astype(BF16)
    q_heads, k_heads, v_heads = qkv_all[0], qkv_all[1], qkv_all[2]
    att_scale = q_heads.shape[-1] ** -0.5
    scores = jnp.einsum('rqnd,rknd->rnqk', q_heads, k_heads, preferred_element_type=F32) * att_scale
    prob_full = jax.nn.softmax(scores, axis=-1)
    prob_half = prob_full.astype(BF16)
    attn_out = jnp.einsum('rnqk,rknd->rqnd', prob_half, v_heads, preferred_element_type=F32).astype(BF16)
    part_out = jnp.einsum('rqnd,ndh->rqh', attn_out, w_out, preferred_element_type=F32)
    return part_out, (q_heads, k_heads, v_heads, prob_full, prob_half, attn_out)


def attn_backward(grad_half, saved_attn, w_qkv, w_out):
    q_heads, k_heads, v_heads, prob_full, prob_half, attn_out = saved_attn
    att_scale = q_heads.shape[-1] ** -0.5
    d_attn = jnp.einsum('rqh,ndh->rqnd', grad_half, w_out, preferred_element_type=F32).astype(BF16)
    d_vals = jnp.einsum('rnqk,rqnd->rknd', prob_half, d_attn, preferred_element_type=F32)
    d_probs = jnp.einsum('rqnd,rknd->rnqk', d_attn, v_heads, preferred_element_type=F32)
    row_dot = jnp.sum(d_probs * prob_full, axis=-1, keepdims=True)
    d_scores = (prob_full * (d_probs - row_dot) * att_scale).astype(BF16)
    d_query = jnp.einsum('rnqk,rknd->rqnd', d_scores, k_heads, preferred_element_type=F32)
    d_keys = jnp.einsum('rnqk,rqnd->rknd', d_scores, q_heads, preferred_element_type=F32)
    d_qkv = jnp.stack([d_query.astype(BF16), d_keys.astype(BF16), d_vals.astype(BF16)])
    norm_part = jnp.einsum('crsnd,hcnd->rsh', d_qkv, w_qkv, preferred_element_type=F32)
    return norm_part.astype(BF16), d_qkv


def solution(mesh):
    act_spec = P('dp')
    in_specs = (act_spec, act_spec, act_spec, act_spec,
                P(None, None, None, 'tp', None), P(None, 'tp', None, None),
                P(None, None, 'tp'), P(None, 'tp', None))
    out_specs = (act_spec, act_spec, act_spec, act_spec,
                 P('dp', None, None, 'tp', None), P('dp', 'tp', None, None),
                 P('dp', None, 'tp'), P('dp', 'tp', None))
    core_swap = [(i, i ^ 1) for i in range(4)]
    chip_swap = [(i, i ^ 2) for i in range(4)]

    def gather_rows(own):
        pair = jnp.concatenate([own, lax.ppermute(own, 'tp', chip_swap)])
        return jnp.concatenate([pair, lax.ppermute(pair, 'tp', core_swap)])

    def scatter_sum(part):
        half = part.shape[0] // 2
        quarter = half // 2
        other = lax.ppermute(part[half:], 'tp', core_swap)
        give = part[quarter:half].astype(F32) + other[quarter:].astype(F32)
        come = lax.ppermute(give.astype(part.dtype), 'tp', chip_swap)
        keep = part[:quarter].astype(F32) + other[:quarter].astype(F32)
        return keep + come.astype(F32)

    def device_body(y_one, y_two, dy_one, dy_two, w_qkv, w_out, w_up, w_down):
        n_micro, n_batch, seq_len, model_dim = y_one.shape
        n_layers = w_qkv.shape[0]
        me = lax.axis_index('tp')
        owners = (me, me ^ 2, me ^ 1, me ^ 3)
        def split(arr):
            return arr.reshape(STREAMS, 4, -1, seq_len, model_dim)

        def own_rows(arr, stream):
            return lax.dynamic_index_in_dim(split(arr)[stream], me, 0, keepdims=False)

        def relative(arr, stream):
            rows = split(arr)[stream]
            return jnp.concatenate([lax.dynamic_index_in_dim(rows, o, 0, keepdims=False) for o in owners])

        def absolute(streams):
            res = []
            for rows in streams:
                slots = rows.reshape(4, -1, seq_len, model_dim)
                for owner in range(4):
                    far = me ^ owner
                    place = (far // 2) + 2 * (far % 2)
                    res.append(lax.dynamic_index_in_dim(slots, place, 0, keepdims=False))
            return jnp.concatenate(res).reshape(y_one.shape)

        stream_ids = range(STREAMS)
        up1 = [own_rows(y_one, s) for s in stream_ids]
        up2 = [own_rows(y_two, s) for s in stream_ids]
        gr1 = [own_rows(dy_one, s) for s in stream_ids]
        gr2 = [own_rows(dy_two, s) for s in stream_ids]
        normed = [rms_norm(relative(y_one, s)).astype(BF16) for s in stream_ids]
        g2_all = [relative(dy_two, s).astype(BF16) for s in stream_ids]
        cat = lambda parts, axis=0: jnp.concatenate(parts, axis=axis) if len(parts) > 1 else parts[0]

        grads_qkv, grads_out, grads_up, grads_down = [], [], [], []
        x1_all = x2_all = d1_all = d2_all = None
        for layer in reversed(range(n_layers)):
            last = layer == 0
            wq, wo, wu, wd = w_qkv[layer], w_out[layer], w_up[layer], w_down[layer]
            low2, normed2, acts, dpres, attns, g1_all, dqkvs, low1 = [], [], [], [], [], [], [], []
            new_g1, new_g2, next_normed, next_g2 = [], [], [], []
            x1_all, x2_all, d1_all, d2_all = [], [], [], []
            for s in stream_ids:
                g_part, saved = mlp_forward(normed[s], wu, wd)
                acts.append(saved)
                low2.append(up2[s] - scatter_sum(g_part))
                if last:
                    x2_all.append(gather_rows(low2[s]))
                    normed2.append(rms_norm(x2_all[s]).astype(BF16))
                else:
                    normed2.append(gather_rows(rms_norm(low2[s]).astype(BF16)))
            for s in stream_ids:
                norm_part, d_pre = mlp_backward(g2_all[s], acts[s], wu, wd)
                dpres.append(d_pre)
                new_g1.append(gr1[s] + norm_back(up1[s], scatter_sum(norm_part)))
                if last:
                    d1_all.append(gather_rows(new_g1[s]))
                    g1_all.append(d1_all[s].astype(BF16))
                else:
                    g1_all.append(gather_rows(new_g1[s].astype(BF16)))
            for s in stream_ids:
                f_part, saved = attn_forward(normed2[s], wq, wo)
                attns.append(saved)
                low1.append(up1[s] - scatter_sum(f_part))
                if last:
                    x1_all.append(gather_rows(low1[s]))
                else:
                    next_normed.append(gather_rows(rms_norm(low1[s]).astype(BF16)))
            for s in stream_ids:
                norm_part, d_qkv = attn_backward(g1_all[s], attns[s], wq, wo)
                dqkvs.append(d_qkv)
                new_g2.append(gr2[s] + norm_back(low2[s], scatter_sum(norm_part)))
                if last:
                    d2_all.append(gather_rows(new_g2[s]))
                else:
                    next_g2.append(gather_rows(new_g2[s].astype(BF16)))
            grads_down.append(jnp.einsum('rsf,rsh->fh', cat([a[0] for a in acts]), cat(g2_all),
                                         preferred_element_type=F32))
            grads_up.append(jnp.einsum('rsh,rsf->hf', cat(normed), cat(dpres), preferred_element_type=F32))
            grads_out.append(jnp.einsum('rqnd,rqh->ndh', cat([a[5] for a in attns]), cat(g1_all),
                                        preferred_element_type=F32))
            grads_qkv.append(jnp.einsum('rsh,crsnd->hcnd', cat(normed2), cat(dqkvs, 1),
                                        preferred_element_type=F32))
            up1, up2, gr1, gr2 = low1, low2, new_g1, new_g2
            normed, g2_all = next_normed, next_g2
        return (absolute(x1_all), absolute(x2_all), absolute(d1_all), absolute(d2_all),
                jnp.stack(grads_qkv[::-1]), jnp.stack(grads_out[::-1]),
                jnp.stack(grads_up[::-1]), jnp.stack(grads_down[::-1]))

    return jax.shard_map(device_body, mesh=mesh, in_specs=in_specs, out_specs=out_specs, check_vma=False)
```

```python
import functools
import math

import jax
import jax.numpy as jnp
from jax import lax
from jax.experimental import pallas as pl
from jax.experimental.pallas import tpu as pltpu
from jax.sharding import PartitionSpec as P

EPS = 1e-6
STREAMS = 2
BF16 = jnp.bfloat16
F32 = jnp.float32
GELU_C = math.sqrt(2.0 / math.pi)
NN = (((1,), (0,)), ((), ()))
NT = (((1,), (1,)), ((), ()))
TN = (((0,), (0,)), ((), ()))


def mm(a, b, dims=NN):
    return lax.dot_general(a, b, dims, preferred_element_type=F32)


def rms_norm(x_in):
    return x_in * lax.rsqrt(jnp.mean(x_in * x_in, axis=-1, keepdims=True) + EPS)


def norm_back(x_in, grad_norm):
    return jax.vjp(rms_norm, x_in)[1](grad_norm)[0]


def whole(arr):
    return pl.BlockSpec(arr.shape, lambda *_: (0,) * len(arr.shape))


def shape_of(*dims, dtype=F32):
    return jax.ShapeDtypeStruct(dims, dtype)


def params():
    return pltpu.CompilerParams(dimension_semantics=("arbitrary",))


def cost(flops, nbytes):
    return pl.CostEstimate(flops=int(flops), bytes_accessed=int(nbytes), transcendentals=0)


def join(refs, out_ref, start=0):
    for ref in refs:
        rows = ref.shape[0]
        out_ref[start:start + rows, :] = ref[...]
        start += rows


def mlp_fwd_kernel(a0, a1, a2, a3, w_up, w_down, keep, send, act, slope, rows):
    step = pl.program_id(0)

    @pl.when(step == 0)
    def _():
        join((a0, a1, a2, a3), rows)

    half = keep.shape[0]
    u = mm(rows[...], w_up[...])
    square = u * u
    t = jnp.tanh(GELU_C * (u + 0.044715 * (square * u)))
    act_half = (0.5 * u * (1.0 + t)).astype(BF16)
    act[...] = act_half
    slope[...] = 0.5 * (1.0 + t) + 0.5 * u * (1.0 - t * t) * (GELU_C * (1.0 + 3 * 0.044715 * square))
    part = mm(act_half, w_down[...])

    @pl.when(step == 0)
    def _():
        keep[...] = part[:half]
        send[...] = part[half:]

    @pl.when(step != 0)
    def _():
        keep[...] += part[:half]
        send[...] += part[half:]


def mlp_fwd(pieces, w_up, w_down, layer, block=512):
    hidden = w_up.shape[1]
    inner = w_up.shape[2]
    rows = sum(p.shape[0] for p in pieces)
    half = rows // 2
    return pl.pallas_call(
        mlp_fwd_kernel,
        grid=(inner // block,),
        in_specs=[whole(p) for p in pieces] + [
            pl.BlockSpec((None, hidden, block), lambda j: (layer, 0, j)),
            pl.BlockSpec((None, block, hidden), lambda j: (layer, j, 0))],
        out_specs=[pl.BlockSpec((half, hidden), lambda j: (0, 0))] * 2 + [
            pl.BlockSpec((rows, block), lambda j: (0, j))] * 2,
        out_shape=[shape_of(half, hidden), shape_of(half, hidden),
                   shape_of(rows, inner, dtype=BF16), shape_of(rows, inner)],
        scratch_shapes=[pltpu.VMEM((rows, hidden), BF16)],
        compiler_params=params(), name="mlp_fwd",
        cost_estimate=cost(4 * rows * hidden * inner, 4 * hidden * inner + 14 * rows * hidden),
    )(*pieces, w_up, w_down)


def mlp_bwd_kernel(a0, a1, a2, a3, w_up, w_down, slope, keep, send, d_pre, rows, total):
    step = pl.program_id(0)

    @pl.when(step == 0)
    def _():
        join((a0, a1, a2, a3), rows)

    half = keep.shape[0]
    d_act = mm(rows[...], w_down[...], NT)
    d_half = (d_act * slope[...]).astype(BF16)
    d_pre[...] = d_half
    part = mm(d_half, w_up[...], NT)

    @pl.when(step == 0)
    def _():
        total[...] = part

    @pl.when(step != 0)
    def _():
        total[...] += part

    @pl.when(step == pl.num_programs(0) - 1)
    def _():
        keep[...] = total[:half, :].astype(BF16)
        send[...] = total[half:, :].astype(BF16)


def mlp_bwd(pieces, w_up, w_down, slope, layer, block=512):
    hidden = w_up.shape[1]
    inner = w_up.shape[2]
    rows = slope.shape[0]
    half = rows // 2
    return pl.pallas_call(
        mlp_bwd_kernel,
        grid=(inner // block,),
        in_specs=[whole(p) for p in pieces] + [
            pl.BlockSpec((None, hidden, block), lambda j: (layer, 0, j)),
            pl.BlockSpec((None, block, hidden), lambda j: (layer, j, 0)),
            pl.BlockSpec((rows, block), lambda j: (0, j))],
        out_specs=[pl.BlockSpec((half, hidden), lambda j: (0, 0))] * 2 + [
            pl.BlockSpec((rows, block), lambda j: (0, j))],
        out_shape=[shape_of(half, hidden, dtype=BF16), shape_of(half, hidden, dtype=BF16),
                   shape_of(rows, inner, dtype=BF16)],
        scratch_shapes=[pltpu.VMEM((rows, hidden), BF16), pltpu.VMEM((rows, hidden), F32)],
        compiler_params=params(), name="mlp_bwd",
        cost_estimate=cost(4 * rows * hidden * inner, 4 * hidden * inner + 14 * rows * hidden),
    )(*pieces, w_up, w_down, slope)


TILE = 128


def attn_fwd_kernel(seq, heads, dim, a0, a1, a2, a3, w_qkv, w_out, keep, send, qkv, attn, prob, rows):
    join((a0, a1, a2, a3), rows)
    n_rows = rows.shape[0]
    half = keep.shape[0]
    width = heads * dim
    qkv[...] = mm(w_qkv[...], rows[...], NT).astype(BF16)
    scale = dim ** -0.5
    r_id = lax.broadcasted_iota(jnp.int32, (TILE, TILE), 0) // seq
    c_id = lax.broadcasted_iota(jnp.int32, (TILE, TILE), 1) // seq
    same = r_id == c_id
    for head in range(heads):
        lo = head * dim
        for tile in range(n_rows // TILE):
            cols = slice(tile * TILE, (tile + 1) * TILE)
            q = qkv[lo:lo + dim, cols]
            k = qkv[width + lo:width + lo + dim, cols]
            v = qkv[2 * width + lo:2 * width + lo + dim, cols]
            scores = jnp.where(same, mm(q, k, TN) * scale, -jnp.inf)
            expo = jnp.exp(scores - jnp.max(scores, axis=-1, keepdims=True))
            p = expo / jnp.sum(expo, axis=-1, keepdims=True)
            prob[head, tile] = p
            attn[lo:lo + dim, cols] = mm(v, p.astype(BF16), NT).astype(BF16)
    keep[...] = mm(attn[:, :half], w_out[...], TN)
    send[...] = mm(attn[:, half:], w_out[...], TN)


def attn_fwd(pieces, w_qkv, w_out, layer, seq, heads, dim):
    hidden = w_qkv.shape[-1]
    rows = sum(p.shape[0] for p in pieces)
    half = rows // 2
    wide, width = 3 * heads * dim, heads * dim
    outs = [shape_of(half, hidden), shape_of(half, hidden), shape_of(wide, rows, dtype=BF16),
            shape_of(width, rows, dtype=BF16), shape_of(heads, rows // TILE, TILE, TILE)]
    return pl.pallas_call(
        functools.partial(attn_fwd_kernel, seq, heads, dim),
        grid=(1,),
        in_specs=[whole(p) for p in pieces] + [
            pl.BlockSpec((None, wide, hidden), lambda j: (layer, 0, 0)),
            pl.BlockSpec((None, width, hidden), lambda j: (layer, 0, 0))],
        out_specs=[whole(o) for o in outs],
        out_shape=outs,
        scratch_shapes=[pltpu.VMEM((rows, hidden), BF16)],
        compiler_params=params(), name="attn_fwd",
        cost_estimate=cost(2 * rows * hidden * (wide + width) * 1.5, 2 * hidden * (wide + width) + 14 * rows * hidden),
    )(*pieces, w_qkv, w_out)


def attn_bwd_kernel(heads, dim, a0, a1, a2, a3, w_qkv, w_out, qkv, prob, keep, send, d_qkv, rows, d_attn):
    join((a0, a1, a2, a3), rows)
    n_rows = rows.shape[0]
    half = keep.shape[0]
    width = heads * dim
    d_attn[...] = mm(w_out[...], rows[...], NT).astype(BF16)
    scale = dim ** -0.5
    for head in range(heads):
        lo = head * dim
        for tile in range(n_rows // TILE):
            cols = slice(tile * TILE, (tile + 1) * TILE)
            q = qkv[lo:lo + dim, cols]
            k = qkv[width + lo:width + lo + dim, cols]
            v = qkv[2 * width + lo:2 * width + lo + dim, cols]
            d_o = d_attn[lo:lo + dim, cols]
            p = prob[head, tile]
            d_qkv[2 * width + lo:2 * width + lo + dim, cols] = mm(d_o, p.astype(BF16)).astype(BF16)
            d_p = mm(d_o, v, TN)
            row_dot = jnp.sum(d_p * p, axis=-1, keepdims=True)
            d_s = (p * (d_p - row_dot) * scale).astype(BF16)
            d_qkv[lo:lo + dim, cols] = mm(k, d_s, NT).astype(BF16)
            d_qkv[width + lo:width + lo + dim, cols] = mm(q, d_s).astype(BF16)
    keep[...] = mm(d_qkv[:, :half], w_qkv[...], TN).astype(BF16)
    send[...] = mm(d_qkv[:, half:], w_qkv[...], TN).astype(BF16)


def attn_bwd(pieces, w_qkv, w_out, qkv, prob, layer, heads, dim):
    hidden = w_qkv.shape[-1]
    rows = qkv.shape[1]
    half = rows // 2
    wide, width = 3 * heads * dim, heads * dim
    outs = [shape_of(half, hidden, dtype=BF16), shape_of(half, hidden, dtype=BF16),
            shape_of(wide, rows, dtype=BF16)]
    return pl.pallas_call(
        functools.partial(attn_bwd_kernel, heads, dim),
        grid=(1,),
        in_specs=[whole(p) for p in pieces] + [
            pl.BlockSpec((None, wide, hidden), lambda j: (layer, 0, 0)),
            pl.BlockSpec((None, width, hidden), lambda j: (layer, 0, 0)), whole(qkv), whole(prob)],
        out_specs=[whole(o) for o in outs],
        out_shape=outs,
        scratch_shapes=[pltpu.VMEM((rows, hidden), BF16), pltpu.VMEM((width, rows), BF16)],
        compiler_params=params(), name="attn_bwd",
        cost_estimate=cost(2 * rows * hidden * (wide + width) * 1.5, 2 * hidden * (wide + width) + 14 * rows * hidden),
    )(*pieces, w_qkv, w_out, qkv, prob)


def grad_mlp_kernel(n_alias, *refs):
    n = STREAMS
    x_refs, dy_refs = refs[:4 * n], refs[4 * n:8 * n]
    pre_refs, act_refs = refs[8 * n:9 * n], refs[9 * n:10 * n]
    d_up, d_down, x_rows, dy_rows = refs[10 * n + n_alias:]

    @pl.when(pl.program_id(0) == 0)
    def _():
        start = 0
        for s in range(n):
            for ref in x_refs[4 * s:4 * s + 4]:
                x_rows[:, start:start + ref.shape[0]] = ref[...].T
                start += ref.shape[0]
        join(dy_refs, dy_rows)

    step_rows = pre_refs[0].shape[0]
    up = down = 0.0
    for s in range(n):
        span = slice(s * step_rows, (s + 1) * step_rows)
        up += mm(x_rows[:, span], pre_refs[s][...])
        down += mm(act_refs[s][...], dy_rows[span, :], TN)
    d_up[...] = up
    d_down[...] = down


def grad_mlp(normed, grads, d_pres, acts, stacks, layer, n_layers, block=256):
    hidden, inner = normed[0][0].shape[1], d_pres[0].shape[1]
    rows = d_pres[0].shape[0]
    flat = [p for pieces in normed for p in pieces] + [p for pieces in grads for p in pieces]
    blocked = list(d_pres) + list(acts)
    args = flat + blocked + list(stacks)
    first = len(flat) + len(blocked)
    return pl.pallas_call(
        functools.partial(grad_mlp_kernel, len(stacks)),
        grid=(inner // block,),
        in_specs=[whole(p) for p in flat] + [pl.BlockSpec((rows, block), lambda j: (0, j))] * len(blocked)
        + [pl.BlockSpec(memory_space=pl.ANY)] * len(stacks),
        out_specs=[pl.BlockSpec((None, hidden, block), lambda j: (layer, 0, j)),
                   pl.BlockSpec((None, block, hidden), lambda j: (layer, j, 0))],
        out_shape=[shape_of(n_layers, hidden, inner), shape_of(n_layers, inner, hidden)],
        scratch_shapes=[pltpu.VMEM((hidden, STREAMS * rows), BF16), pltpu.VMEM((STREAMS * rows, hidden), BF16)],
        input_output_aliases={first + i: i for i in range(len(stacks))},
        compiler_params=params(), name="grad_mlp",
        cost_estimate=cost(4 * STREAMS * rows * hidden * inner, 8 * hidden * inner + 8 * STREAMS * rows * hidden),
    )(*args)


def grad_attn_kernel(n_alias, *refs):
    n = STREAMS
    x_refs, dy_refs = refs[:4 * n], refs[4 * n:8 * n]
    qkv_refs, attn_refs = refs[8 * n:9 * n], refs[9 * n:10 * n]
    d_wqkv, d_wout, x_rows, dy_rows = refs[10 * n + n_alias:]

    @pl.when(pl.program_id(0) == 0)
    def _():
        join(x_refs, x_rows)
        join(dy_refs, dy_rows)

    step_rows = qkv_refs[0].shape[1]
    first = second = 0.0
    for s in range(n):
        span = slice(s * step_rows, (s + 1) * step_rows)
        first += mm(qkv_refs[s][...], x_rows[span, :])
        second += mm(attn_refs[s][...], dy_rows[span, :])
    d_wqkv[...] = first
    d_wout[...] = second


def grad_attn(normed, grads, d_qkvs, attns, stacks, layer, n_layers, steps=3):
    hidden = normed[0][0].shape[1]
    wide, rows = d_qkvs[0].shape
    width = attns[0].shape[0]
    flat = [p for pieces in normed for p in pieces] + [p for pieces in grads for p in pieces]
    args = flat + list(d_qkvs) + list(attns) + list(stacks)
    first = len(flat) + 2 * STREAMS
    return pl.pallas_call(
        functools.partial(grad_attn_kernel, len(stacks)),
        grid=(steps,),
        in_specs=[whole(p) for p in flat] + [pl.BlockSpec((wide // steps, rows), lambda j: (j, 0))] * STREAMS
        + [pl.BlockSpec((width // steps, rows), lambda j: (j, 0))] * STREAMS
        + [pl.BlockSpec(memory_space=pl.ANY)] * len(stacks),
        out_specs=[pl.BlockSpec((None, wide // steps, hidden), lambda j: (layer, j, 0)),
                   pl.BlockSpec((None, width // steps, hidden), lambda j: (layer, j, 0))],
        out_shape=[shape_of(n_layers, wide, hidden), shape_of(n_layers, width, hidden)],
        scratch_shapes=[pltpu.VMEM((STREAMS * rows, hidden), BF16)] * 2,
        input_output_aliases={first + i: i for i in range(len(stacks))},
        compiler_params=params(), name="grad_attn",
        cost_estimate=cost(2 * STREAMS * rows * hidden * (wide + width), 4 * hidden * (wide + width) + 8 * STREAMS * rows * hidden),
    )(*args)


def solution(mesh):
    act_spec = P('dp')
    in_specs = (act_spec, act_spec, act_spec, act_spec,
                P(None, None, None, 'tp', None), P(None, 'tp', None, None),
                P(None, None, 'tp'), P(None, 'tp', None))
    out_specs = (act_spec, act_spec, act_spec, act_spec,
                 P('dp', None, None, 'tp', None), P('dp', 'tp', None, None),
                 P('dp', None, 'tp'), P('dp', 'tp', None))
    core_swap = [(i, i ^ 1) for i in range(4)]
    chip_swap = [(i, i ^ 2) for i in range(4)]

    def gather_rows(own):
        chip = lax.ppermute(own, 'tp', chip_swap)
        return (own, chip, lax.ppermute(own, 'tp', core_swap), lax.ppermute(chip, 'tp', core_swap))

    def scatter_sum(keep, send):
        quarter = keep.shape[0] // 2
        other = lax.ppermute(send, 'tp', core_swap)
        give = keep[quarter:].astype(F32) + other[quarter:].astype(F32)
        come = lax.ppermute(give.astype(keep.dtype), 'tp', chip_swap)
        mine = keep[:quarter].astype(F32) + other[:quarter].astype(F32)
        return mine + come.astype(F32)

    def device_body(y_one, y_two, dy_one, dy_two, w_qkv, w_out, w_up, w_down):
        hidden = y_one.shape[-1]
        seq = y_one.shape[2]
        n_layers, _, _, heads, dim = w_qkv.shape
        wq_t = jnp.transpose(w_qkv, (0, 2, 3, 4, 1)).reshape(n_layers, 3 * heads * dim, hidden)
        wo_t = w_out.reshape(n_layers, heads * dim, hidden)
        me = lax.axis_index('tp')
        owners = (me, me ^ 2, me ^ 1, me ^ 3)

        def split(arr):
            return arr.reshape(STREAMS, 4, -1, hidden)

        def pick(arr, stream, owner):
            return lax.dynamic_index_in_dim(split(arr)[stream], owner, 0, keepdims=False)

        def absolute(streams):
            res = []
            for pieces in streams:
                slots = jnp.stack(pieces)
                for owner in range(4):
                    far = me ^ owner
                    place = (far >> 1) | ((far & 1) << 1)
                    res.append(lax.dynamic_index_in_dim(slots, place, 0, keepdims=False))
            return jnp.concatenate(res).reshape(y_one.shape)

        ids = range(STREAMS)
        up1 = [pick(y_one, s, me) for s in ids]
        up2 = [pick(y_two, s, me) for s in ids]
        gr1 = [pick(dy_one, s, me) for s in ids]
        gr2 = [pick(dy_two, s, me) for s in ids]
        normed = [[rms_norm(pick(y_one, s, o)).astype(BF16) for o in owners] for s in ids]
        g2_all = [[pick(dy_two, s, o).astype(BF16) for o in owners] for s in ids]
        to_half = lambda pieces: [p.astype(BF16) for p in pieces]
        to_norm = lambda pieces: [rms_norm(p).astype(BF16) for p in pieces]

        mlp_stacks, attn_stacks = (), ()
        x1_all = x2_all = d1_all = d2_all = None
        for layer in reversed(range(n_layers)):
            last = layer == 0
            low2, normed2, saved_m, d_pres, saved_a, g1_all, d_qkvs, low1 = [], [], [], [], [], [], [], []
            new_g1, new_g2, next_normed, next_g2 = [], [], [], []
            x1_all, x2_all, d1_all, d2_all = [], [], [], []
            for s in ids:
                keep, send, act, slope = mlp_fwd(normed[s], w_up, w_down, layer)
                saved_m.append((act, slope))
                low2.append(up2[s] - scatter_sum(keep, send))
                if last:
                    x2_all.append(gather_rows(low2[s]))
                    normed2.append(to_norm(x2_all[s]))
                else:
                    normed2.append(gather_rows(rms_norm(low2[s]).astype(BF16)))
            for s in ids:
                keep, send, d_pre = mlp_bwd(g2_all[s], w_up, w_down, saved_m[s][1], layer)
                d_pres.append(d_pre)
                new_g1.append(gr1[s] + norm_back(up1[s], scatter_sum(keep, send)))
                if last:
                    d1_all.append(gather_rows(new_g1[s]))
                    g1_all.append(to_half(d1_all[s]))
                else:
                    g1_all.append(gather_rows(new_g1[s].astype(BF16)))
            for s in ids:
                keep, send, qkv, attn, prob = attn_fwd(normed2[s], wq_t, wo_t, layer, seq, heads, dim)
                saved_a.append((qkv, attn, prob))
                low1.append(up1[s] - scatter_sum(keep, send))
                if last:
                    x1_all.append(gather_rows(low1[s]))
                else:
                    next_normed.append(gather_rows(rms_norm(low1[s]).astype(BF16)))
            for s in ids:
                keep, send, d_qkv = attn_bwd(g1_all[s], wq_t, wo_t, saved_a[s][0], saved_a[s][2], layer, heads, dim)
                d_qkvs.append(d_qkv)
                new_g2.append(gr2[s] + norm_back(low2[s], scatter_sum(keep, send)))
                if last:
                    d2_all.append(gather_rows(new_g2[s]))
                else:
                    next_g2.append(gather_rows(new_g2[s].astype(BF16)))
            mlp_stacks = grad_mlp(normed, g2_all, d_pres, [m[0] for m in saved_m], mlp_stacks, layer, n_layers)
            attn_stacks = grad_attn(normed2, g1_all, d_qkvs, [a[1] for a in saved_a], attn_stacks, layer, n_layers)
            up1, up2, gr1, gr2 = low1, low2, new_g1, new_g2
            normed, g2_all = next_normed, next_g2
        d_wqkv = jnp.transpose(attn_stacks[0].reshape(n_layers, 3, heads, dim, hidden), (0, 4, 1, 2, 3))
        return (absolute(x1_all), absolute(x2_all), absolute(d1_all), absolute(d2_all),
                d_wqkv, attn_stacks[1].reshape(w_out.shape), mlp_stacks[0], mlp_stacks[1])

    return jax.shard_map(device_body, mesh=mesh, in_specs=in_specs, out_specs=out_specs, check_vma=False)
```
